32 devices in a mesh: tok: 8 (over y, x, core), col: 4 (over z).
Axes of the slice: x: 2, y: 2, z: 4, core: 2. Of those that a mesh axis runs over, the one named last changes fastest.
Arguments:
- acts_a: bfloat16 [8192, 3584], P('tok', 'col'), may hold values from -6 to 6
- acts_b: bfloat16 [8192, 4096], P('tok', 'col'), may hold values from -6 to 6
- whiten_a: bfloat16 [3584, 3584], P(None, 'col'), may hold values from -0.09375 to 0.09375
- whiten_b: bfloat16 [4096, 4096], P(None, 'col'), may hold values from -0.09375 to 0.09375
Outputs:
- cross: float32 [3584, 4096], P('col', 'tok')
The draws below stay inside these ranges and needn't reach their ends.
All inputs are finite; a program needn't handle non-finite values.
Results may differ from the reference program's by a relative error of at most 0.0041.
Values may be sent and summed in bfloat16 or wider, within the bound.
No kernel may reach another device: no remote copies, remote signals or barrier semaphores. Data moves between devices by JAX's collectives and lax.ppermute only.
A program may use at most 128 MiB of HBM per device.

```python
import jax
import jax.numpy as jnp
from jax import lax

DA = 3584
DB = 4096
TOKENS = 8192


def shard_levels(own_key, shape, pieces, low, top_value):
    def one(dim, shards_of):
        heights = jax.random.uniform(jax.random.fold_in(jax.random.fold_in(own_key, 6), dim), (shards_of,), jnp.float32, low / len(pieces), top_value / len(pieces))
        return jnp.repeat(jnp.exp(heights), shape[dim] // shards_of).reshape((-1,) + (1,) * (len(shape) - dim - 1))

    loudness = one(*pieces[0])
    for cut in pieces[1:]:
        loudness = loudness * one(*cut)
    return loudness


def bell_draw(key, shape, spread, bound, shards=(), held_as=jnp.bfloat16):
    drawn = jax.random.normal(key, shape, jnp.float32) * spread
    if len(shards) > 0:
        drawn = shard_levels(key, shape, shards, -0.22, 0.18) * drawn
    return jnp.clip(drawn, min=-bound, max=bound).astype(held_as)


def setup_inputs(seed: int = 0) -> dict:
    streams_of = jax.random.split(jax.random.key(seed), 5)
    acts_a = bell_draw(streams_of[0], (TOKENS, DA), 1.0, 6.0, ((0, 8), (1, 4)))
    acts_b = bell_draw(streams_of[1], (TOKENS, DB), 1.0, 6.0, ((0, 8), (1, 4)))
    whiten_a = bell_draw(streams_of[2], (DA, DA), DA ** -0.5, 0.09375, ((1, 4),))
    whiten_b = bell_draw(streams_of[3], (DB, DB), DB ** -0.5, 0.09375, ((1, 4),))
    return {"acts_a": acts_a, "acts_b": acts_b, "whiten_a": whiten_a, "whiten_b": whiten_b}


def reference(acts_a, acts_b, whiten_a, whiten_b):
    white_a = jnp.dot(acts_a, whiten_a, preferred_element_type=jnp.float32).astype(jnp.bfloat16)
    white_b = jnp.dot(acts_b, whiten_b, preferred_element_type=jnp.float32).astype(jnp.bfloat16)
    summed = lax.dot_general(white_a, white_b, (((0,), (0,)), ((), ())), preferred_element_type=jnp.float32)
    scale = 1.0 / jnp.sqrt(jnp.float32(TOKENS))
    return summed * scale
```

```python
import jax
import jax.numpy as jnp
from jax import lax
from jax.sharding import PartitionSpec as P

PIECES = 2
LANES = 128


def cuts(width):
    groups = width // LANES
    if width % LANES or groups < PIECES:
        return [(0, width)]
    sizes = [groups // PIECES + (i < groups % PIECES) for i in range(PIECES)]
    ranges, at = [], 0
    for size in sizes:
        ranges.append((at * LANES, size * LANES))
        at += size
    return ranges


def halve(part, bit, sent_as):
    size = lax.axis_size("tok")
    mine = (lax.axis_index("tok") >> bit) & 1
    pairs = [(i, i ^ (1 << bit)) for i in range(size)]
    give = lax.dynamic_index_in_dim(part, 1 - mine, 0, keepdims=False)
    keep = lax.dynamic_index_in_dim(part, mine, 0, keepdims=False)
    got = lax.ppermute(give.astype(sent_as), "tok", pairs)
    return keep + got.astype(jnp.float32)


def reduce_rows(part):
    size = lax.axis_size("tok")
    bits = size.bit_length() - 1
    rows, n = part.shape
    block = part.reshape((2,) * bits + (rows // size, n))
    left = list(range(bits - 1, -1, -1))

    def step(block, left, bit, sent_as):
        at = left.index(bit)
        return halve(jnp.moveaxis(block, at, 0), bit, sent_as), left[:at] + left[at + 1 :]

    block, left = step(block, left, 0, jnp.float32)
    halves = []
    for h, piece in enumerate(jnp.split(block, 2, axis=-1)):
        order = left if h == 0 else left[::-1]
        rest = left
        for bit in order:
            piece, rest = step(piece, rest, bit, jnp.bfloat16)
        halves.append(piece)
    return jnp.concatenate(halves, axis=-1)


def body(acts_a, acts_b, whiten_a, whiten_b):
    toks, cols = lax.axis_size("tok"), lax.axis_size("col")
    width = acts_a.shape[1]
    maps_a = whiten_a.reshape(cols, width, whiten_a.shape[1])
    pieces = cuts(width)
    wides = [
        lax.all_gather(acts_a[:, start : start + size], "col", axis=1, tiled=True)
        for start, size in pieces
    ]
    grams = []
    for wide in wides:
        if grams:
            wide, _ = lax.optimization_barrier((wide, grams[-1]))
        part = lax.dot_general(
            wide, acts_b, (((0,), (0,)), ((), ())), preferred_element_type=jnp.float32
        )
        grams.append(reduce_rows(part).astype(jnp.bfloat16))
    total = None
    for (start, size), gram in zip(pieces, grams):
        gram = lax.all_gather(gram, "col", axis=1, tiled=True)
        right = jnp.dot(gram, whiten_b, preferred_element_type=jnp.float32).astype(jnp.bfloat16)
        right = lax.all_gather(right, "col", axis=1, tiled=True)
        right = lax.all_to_all(right, "tok", split_axis=1, concat_axis=0, tiled=True)
        left = maps_a[:, start : start + size].reshape(cols * size, -1)
        term = lax.dot_general(
            left, right, (((0,), (0,)), ((), ())), preferred_element_type=jnp.float32
        )
        total = term if total is None else total + term
    scale = 1.0 / jnp.sqrt(jnp.float32(acts_a.shape[0] * toks))
    return total * scale


def solution(mesh):
    placed = (P("tok", "col"), P("tok", "col"), P(None, "col"), P(None, "col"))
    return jax.shard_map(
        body, mesh=mesh, in_specs=placed, out_specs=P("col", "tok"), check_vma=False
    )
```
